32 devices in a mesh: replica: 8 (over z, y), shard: 4 (over x, core).
Axes of the slice: x: 2, y: 2, z: 4, core: 2. Of those that a mesh axis runs over, the one named last changes fastest.
Arguments:
- outer_params: float32 [512, 4096], P('shard'), may hold values from -6 to 6, as said below
- local_params: bfloat16 [8, 512, 4096], P('replica', 'shard'), may hold values from -70 to 70
- momentum: float32 [512, 4096], P('shard'), may hold values from -6 to 6
Outputs:
- params_next: float32 [512, 4096], P('shard')
- momentum_next: float32 [512, 4096], P('shard')
- block_scales: float32 [32, 512], P(None, 'shard')
The draws below stay inside these ranges and needn't reach their ends.
Inputs may be any that keep to these rules, and one draw needn't show every extreme that they name: `outer_params`: outer parameters of order one.
All inputs are finite; a program needn't handle non-finite values.
Results may differ from the reference program's by a relative error of at most 0.005.
Values may be sent and summed in bfloat16 or wider, within the bound.
A program may use at most 64 MiB of HBM per device.

```python
import math
import jax
import jax.numpy as jnp
from jax import lax

D = 4096
BLOCK = 128
ROWS = 512
WORKERS = 8


def draw_fields(key):
    base_key = jax.random.fold_in(key, 71)
    outer_key = jax.random.fold_in(base_key, 1)
    column_key = jax.random.fold_in(base_key, 2)
    common_key = jax.random.fold_in(base_key, 3)
    noise_key = jax.random.fold_in(base_key, 4)
    level_key = jax.random.fold_in(base_key, 5)
    group_rows = 32
    group_count = (ROWS + group_rows - 1) // group_rows
    raw_levels = jax.random.uniform(level_key, (group_count,), jnp.float32, 0.0, 1.0)
    unit_levels = raw_levels - jnp.max(raw_levels) + 1.0
    row_group = jnp.arange(ROWS, dtype=jnp.int32) // group_rows
    row_scale = 10.0 ** unit_levels[row_group]
    common_part = jnp.clip(jax.random.normal(common_key, (ROWS, D), jnp.float32), -4.0, 4.0)
    noise_part = jnp.clip(jax.random.normal(noise_key, (WORKERS, ROWS, D), jnp.float32), -4.0, 4.0)
    column_scale = jnp.exp(jax.random.uniform(column_key, (D,), jnp.float32, 0.0, math.log(10.0)))
    outer_values = jnp.clip(jax.random.normal(outer_key, (ROWS, D), jnp.float32), -6.0, 6.0)
    deltas = 0.05 * row_scale[:, None] * column_scale[None, :] * (common_part[None] + noise_part)
    return (outer_values, deltas)


def draw_outer_params(key, part):
    outer_values, deltas = draw_fields(key)
    return outer_values


def draw_local_params(key, part):
    outer_values, deltas = draw_fields(key)
    return (outer_values[None] - deltas).astype(jnp.bfloat16)


def block_scale(stream_key, extent, pieces, low, high):
    level = 1.0
    for axis_at, shards_of in pieces:
        draws = jax.random.uniform(jax.random.fold_in(jax.random.fold_in(stream_key, 6), axis_at), (shards_of,), jnp.float32, low / len(pieces), high / len(pieces))
        level = level * jnp.repeat(jnp.exp(draws), extent[axis_at] // shards_of).reshape((-1,) + (1,) * (len(extent) - 1 - axis_at))
    return level


def scatter_about(stream_key, dims, scale, most, pieces=(), kind=jnp.bfloat16):
    values = jax.random.normal(stream_key, dims, jnp.float32) * scale
    if len(pieces) > 0:
        values = block_scale(stream_key, dims, pieces, -0.22, 0.18) * values
    return jnp.clip(values, min=-most, max=most).astype(kind)


def setup_inputs(seed: int = 0) -> dict:
    seeds = jax.random.split(jax.random.key(seed), 4)
    outer_params = draw_outer_params(jax.random.fold_in(seeds[3], 71), 0)
    local_params = draw_local_params(jax.random.fold_in(seeds[3], 71), 0)
    momentum = scatter_about(seeds[2], (ROWS, D), 1.0, 6.0, ((0, 4),), jnp.float32)
    return {"outer_params": outer_params, "local_params": local_params, "momentum": momentum}


epsilon = 1e-06
clip_level = 0.5
outer_rate = 0.7
outer_decay = 0.9
grid_levels = 7.0

def smooth_step(values):
    return values - jnp.sin(2.0 * math.pi * values) / (2.0 * math.pi)

def smooth_round(values):
    return smooth_step(smooth_step(values))

def block_max(values):
    return lax.optimization_barrier(jnp.max(jnp.abs(values).reshape(values.shape[0], D // BLOCK, BLOCK), axis=2))

def reference(outer_params, local_params, momentum):

    def worker_max(running, worker_local):
        deltas = outer_params - worker_local.astype(jnp.float32)
        return (jnp.maximum(running, block_max(deltas)), None)
    absmax, _ = lax.scan(worker_max, jnp.zeros((ROWS, D // BLOCK), jnp.float32), local_params)
    spread_scale = jnp.repeat(absmax + epsilon, BLOCK, axis=1)

    def worker_sum(running, worker_local):
        deltas = outer_params - worker_local.astype(jnp.float32)
        encoded = smooth_round(grid_levels * deltas / spread_scale).astype(jnp.bfloat16)
        return (running + spread_scale * encoded.astype(jnp.float32) / grid_levels, None)
    summed_rows, _ = lax.scan(worker_sum, jnp.zeros((ROWS, D), jnp.float32), local_params)
    gradient = summed_rows / WORKERS
    root_mean = jnp.sqrt(jnp.mean(gradient * gradient) + epsilon)
    factor = jnp.minimum(1.0, clip_level / root_mean)
    clipped = factor * gradient
    momentum_next = outer_decay * momentum + clipped
    params_next = outer_params - outer_rate * (clipped + outer_decay * momentum_next)
    return (params_next, momentum_next, absmax.T)
```

```python
import functools

import jax
import jax.numpy as jnp
from jax import lax
from jax.experimental import pallas as pl
from jax.experimental.pallas import tpu as pltpu
from jax.sharding import PartitionSpec as P

BLOCK = 128
MESH = pl.DeviceIdType.MESH

epsilon = 1e-06
clip_level = 0.5
outer_rate = 0.7
outer_decay = 0.9
grid_levels = 7.0

SMOOTH = (6.57973588, -12.98785441, 12.20756634, -6.687892761, 2.368806331, -0.5120006377)
SHIFT = 1.5 * 2.0**23


def smooth_rest(rest):
    square = rest * rest
    value = SMOOTH[-1]
    for coefficient in SMOOTH[-2::-1]:
        value = value * square + coefficient
    return rest * square * value


def column_of(row):
    return jnp.broadcast_to(row, (BLOCK, row.shape[1])).T


def exchange_kernel(
    workers, shards, entry_count,
    outer_hbm, local_hbm, grad_out, max_out, factor_out,
    outer_v, local_v, max_slots, inverse, spread, encoded, arrived, total, share, squares, shard_squares,
    load_sem, max_send, max_recv, enc_send, enc_recv, sq_send, sq_recv, ss_send, ss_recv, gat_send, gat_recv, own_sem,
):
    me = lax.axis_index("replica")
    my_shard = lax.axis_index("shard")
    rows, cols = outer_v.shape
    blocks = cols // BLOCK
    width = cols // workers
    blocks_each = width // BLOCK
    pieces = load_sem.shape[1]
    piece = cols // pieces

    def peer(step):
        return lax.rem(me + step, workers)

    def origin(step):
        return lax.rem(me + workers - step, workers)

    def loads(i):
        part = pl.ds(i * piece, piece)
        return (
            pltpu.make_async_copy(outer_hbm.at[:, part], outer_v.at[:, part], load_sem.at[0, i]),
            pltpu.make_async_copy(local_hbm.at[0, :, part], local_v.at[:, part], load_sem.at[1, i]),
        )

    for i in range(pieces):
        for copy in loads(i):
            copy.start()

    barrier = pltpu.get_barrier_semaphore()

    @pl.loop(1, workers)
    def _(step):
        pl.semaphore_signal(barrier, inc=1, device_id={"replica": peer(step)}, device_id_type=MESH)

    @pl.loop(1, shards)
    def _(step):
        pl.semaphore_signal(
            barrier, inc=1, device_id={"shard": lax.rem(my_shard + step, shards)}, device_id_type=MESH
        )

    def delta(block):
        at = pl.ds(pl.multiple_of(block * BLOCK, BLOCK), BLOCK)
        return outer_v[:, at] - local_v[:, at].astype(jnp.float32)

    per_piece = piece // BLOCK
    for i in range(pieces):
        for copy in loads(i):
            copy.wait()

        @pl.loop(i * per_piece, (i + 1) * per_piece)
        def _(block):
            max_slots[me, pl.ds(block, 1), :] = jnp.max(jnp.abs(delta(block)).T, axis=0, keepdims=True)

    pl.semaphore_wait(barrier, workers + shards - 2)

    def max_copy(step):
        return pltpu.make_async_remote_copy(
            src_ref=max_slots.at[me], dst_ref=max_slots.at[me],
            send_sem=max_send.at[step], recv_sem=max_recv.at[step],
            device_id={"replica": peer(step)}, device_id_type=MESH,
        )

    @pl.loop(1, workers)
    def _(step):
        max_copy(step).start()

    @pl.loop(1, workers)
    def _(step):
        max_copy(step).wait()

    absmax = max_slots[0]
    for w in range(1, workers):
        absmax = jnp.maximum(absmax, max_slots[w])
    max_out[...] = absmax
    inverse[...] = grid_levels / (absmax + epsilon)
    spread[...] = (absmax + epsilon) / (grid_levels * workers)

    def encode(target, put):
        for i in range(blocks_each):
            block = target * blocks_each + i
            values = delta(block) * column_of(inverse[pl.ds(block, 1), :])
            nearest = (values + SHIFT) - SHIFT
            rest = smooth_rest(smooth_rest(values - nearest))
            put(i, (nearest + rest).astype(jnp.bfloat16))

    def enc_copy(step):
        return pltpu.make_async_remote_copy(
            src_ref=encoded.at[peer(step)], dst_ref=arrived.at[me],
            send_sem=enc_send.at[step], recv_sem=enc_recv.at[step],
            device_id={"replica": peer(step)}, device_id_type=MESH,
        )

    @pl.loop(1, workers)
    def _(step):
        target = peer(step)

        def put(i, value):
            encoded[target, :, i * BLOCK : (i + 1) * BLOCK] = value

        encode(target, put)

        @pl.when(step > 1)
        def _():
            enc_copy(step - 1).start()

    def put_own(i, value):
        total[:, i * BLOCK : (i + 1) * BLOCK] = value.astype(jnp.float32)

    encode(me, put_own)
    enc_copy(workers - 1).start()

    @pl.loop(1, workers)
    def _(step):
        enc_copy(step).wait()
        total[...] += arrived[origin(step)].astype(jnp.float32)

    square = jnp.zeros((8, BLOCK), jnp.float32)
    for i in range(blocks_each):
        block = me * blocks_each + i
        value = total[:, i * BLOCK : (i + 1) * BLOCK] * column_of(spread[pl.ds(block, 1), :])
        share[:, i * BLOCK : (i + 1) * BLOCK] = value.astype(jnp.bfloat16)
        square = square + jnp.sum((value * value).reshape(rows // 8, 8, BLOCK), axis=0)
    squares[me] = jnp.broadcast_to(jnp.sum(square, axis=0, keepdims=True), (8, BLOCK))

    def sq_copy(step):
        return pltpu.make_async_remote_copy(
            src_ref=squares.at[me], dst_ref=squares.at[me],
            send_sem=sq_send.at[step], recv_sem=sq_recv.at[step],
            device_id={"replica": peer(step)}, device_id_type=MESH,
        )

    def place(worker):
        return grad_out.at[:, pl.ds(pl.multiple_of(worker * width, BLOCK), width)]

    def gat_copy(step):
        return pltpu.make_async_remote_copy(
            src_ref=share, dst_ref=place(me),
            send_sem=gat_send.at[step], recv_sem=gat_recv.at[step],
            device_id={"replica": peer(step)}, device_id_type=MESH,
        )

    @pl.loop(1, workers)
    def _(step):
        sq_copy(step).start()

    @pl.loop(1, workers)
    def _(step):
        gat_copy(step).start()

    own = pltpu.make_async_copy(share, place(me), own_sem)
    own.start()

    @pl.loop(1, workers)
    def _(step):
        sq_copy(step).wait()

    part = squares[0]
    for w in range(1, workers):
        part = part + squares[w]
    shard_squares[my_shard] = part

    def ss_copy(step):
        return pltpu.make_async_remote_copy(
            src_ref=shard_squares.at[my_shard], dst_ref=shard_squares.at[my_shard],
            send_sem=ss_send.at[step], recv_sem=ss_recv.at[step],
            device_id={"shard": lax.rem(my_shard + step, shards)}, device_id_type=MESH,
        )

    @pl.loop(1, shards)
    def _(step):
        ss_copy(step).start()

    @pl.loop(1, shards)
    def _(step):
        ss_copy(step).wait()

    part = shard_squares[0]
    for s in range(1, shards):
        part = part + shard_squares[s]
    mean = jnp.sum(part, axis=1, keepdims=True) / entry_count
    root_mean = jnp.sqrt(mean + epsilon)
    factor_out[...] = jnp.broadcast_to(jnp.minimum(1.0, clip_level / root_mean), factor_out.shape)

    own.wait()

    @pl.loop(1, workers)
    def _(step):
        gat_copy(step).wait()


def exchange(outer_params, local_params):
    workers = lax.axis_size("replica")
    shards = lax.axis_size("shard")
    rows, cols = outer_params.shape
    blocks = cols // BLOCK
    width = cols // workers
    dma = pltpu.SemaphoreType.DMA
    vmem = pl.BlockSpec(memory_space=pltpu.VMEM)
    anywhere = pl.BlockSpec(memory_space=pl.ANY)
    return pl.pallas_call(
        functools.partial(exchange_kernel, workers, shards, rows * shards * cols),
        out_shape=(
            jax.ShapeDtypeStruct((rows, cols), jnp.bfloat16),
            jax.ShapeDtypeStruct((blocks, rows), jnp.float32),
            jax.ShapeDtypeStruct((8, BLOCK), jnp.float32),
        ),
        in_specs=[anywhere, anywhere],
        out_specs=(anywhere, vmem, vmem),
        scratch_shapes=[
            pltpu.VMEM((rows, cols), jnp.float32),
            pltpu.VMEM((rows, cols), jnp.bfloat16),
            pltpu.VMEM((workers, blocks, rows), jnp.float32),
            pltpu.VMEM((blocks, rows), jnp.float32),
            pltpu.VMEM((blocks, rows), jnp.float32),
            pltpu.VMEM((workers, rows, width), jnp.bfloat16),
            pltpu.VMEM((workers, rows, width), jnp.bfloat16),
            pltpu.VMEM((rows, width), jnp.float32),
            pltpu.VMEM((rows, width), jnp.bfloat16),
            pltpu.VMEM((workers, 8, BLOCK), jnp.float32),
            pltpu.VMEM((shards, 8, BLOCK), jnp.float32),
            dma((2, 4)),
            dma((workers,)), dma((workers,)),
            dma((workers,)), dma((workers,)),
            dma((workers,)), dma((workers,)),
            dma((shards,)), dma((shards,)),
            dma((workers,)), dma((workers,)),
            dma(()),
        ],
        compiler_params=pltpu.CompilerParams(
            collective_id=0, has_side_effects=True, vmem_limit_bytes=16 * 2**20
        ),
        cost_estimate=pl.CostEstimate(
            flops=50 * rows * cols, bytes_accessed=8 * rows * cols * 4, transcendentals=0
        ),
    )(outer_params, local_params)


def per_device(outer_params, local_params, momentum):
    gradient, absmax, factor = exchange(outer_params, local_params)
    clipped = factor[0, 0] * gradient.astype(jnp.float32)
    momentum_next = outer_decay * momentum + clipped
    params_next = outer_params - outer_rate * (clipped + outer_decay * momentum_next)
    return (params_next, momentum_next, absmax)


def solution(mesh):
    return jax.shard_map(
        per_device,
        mesh=mesh,
        in_specs=(P("shard", None), P("replica", "shard", None), P("shard", None)),
        out_specs=(P("shard", None), P("shard", None), P(None, "shard")),
        check_vma=False,
    )
```

```python
import functools

import jax
import jax.numpy as jnp
from jax import lax
from jax.experimental import pallas as pl
from jax.experimental.pallas import tpu as pltpu
from jax.sharding import PartitionSpec as P

BLOCK = 128
MESH = pl.DeviceIdType.MESH

epsilon = 1e-06
clip_level = 0.5
outer_rate = 0.7
outer_decay = 0.9
grid_levels = 7.0

SMOOTH = (6.57973588, -12.98785441, 12.20756634, -6.687892761, 2.368806331, -0.5120006377)
SHIFT = 1.5 * 2.0**23


def smooth_rest(rest):
    square = rest * rest
    value = SMOOTH[-1]
    for coefficient in SMOOTH[-2::-1]:
        value = value * square + coefficient
    return rest * square * value


def column_of(row):
    return jnp.broadcast_to(row, (BLOCK, row.shape[1])).T


def exchange_kernel(
    workers, shards, entry_count,
    outer_hbm, local_hbm, momentum_hbm, grad_out, momentum_out, max_out, factor_out,
    outer_v, local_v, max_slots, inverse, spread, encoded, arrived, total, share, squares, shard_squares,
    load_sem, max_send, max_recv, enc_send, enc_recv, sq_send, sq_recv, ss_send, ss_recv, gat_send, gat_recv, fwd_send, fwd_recv, own_sem, momentum_sem,
):
    me = lax.axis_index("replica")
    my_shard = lax.axis_index("shard")
    rows, cols = outer_v.shape
    blocks = cols // BLOCK
    width = cols // workers
    blocks_each = width // BLOCK
    parts, half = share.shape[:2]
    pieces = load_sem.shape[1]
    piece = cols // pieces

    def peer(step):
        return lax.rem(me + step, workers)

    def origin(step):
        return lax.rem(me + workers - step, workers)

    def loads(i):
        part = pl.ds(i * piece, piece)
        return (
            pltpu.make_async_copy(outer_hbm.at[:, part], outer_v.at[:, part], load_sem.at[0, i]),
            pltpu.make_async_copy(local_hbm.at[0, :, part], local_v.at[:, part], load_sem.at[1, i]),
        )

    for i in range(pieces):
        for copy in loads(i):
            copy.start()
    momentum_copy = pltpu.make_async_copy(momentum_hbm, momentum_out, momentum_sem)

    barrier = pltpu.get_barrier_semaphore()

    @pl.loop(1, workers)
    def _(step):
        pl.semaphore_signal(barrier, inc=1, device_id={"replica": peer(step)}, device_id_type=MESH)

    @pl.loop(1, shards)
    def _(step):
        pl.semaphore_signal(
            barrier, inc=1, device_id={"shard": lax.rem(my_shard + step, shards)}, device_id_type=MESH
        )

    def delta(block, rows_at=slice(None)):
        at = pl.ds(pl.multiple_of(block * BLOCK, BLOCK), BLOCK)
        return outer_v[rows_at, at] - local_v[rows_at, at].astype(jnp.float32)

    per_piece = piece // BLOCK
    for i in range(pieces):
        for copy in loads(i):
            copy.wait()

        @pl.loop(i * per_piece, (i + 1) * per_piece)
        def _(block):
            max_slots[me, pl.ds(block, 1), :] = jnp.max(jnp.abs(delta(block)).T, axis=0, keepdims=True)

    momentum_copy.start()
    pl.semaphore_wait(barrier, workers + shards - 2)

    def max_copy(step):
        return pltpu.make_async_remote_copy(
            src_ref=max_slots.at[me], dst_ref=max_slots.at[me],
            send_sem=max_send.at[step], recv_sem=max_recv.at[step],
            device_id={"replica": peer(step)}, device_id_type=MESH,
        )

    @pl.loop(1, workers)
    def _(step):
        max_copy(step).start()

    @pl.loop(1, workers)
    def _(step):
        max_copy(step).wait()

    absmax = max_slots[0]
    for w in range(1, workers):
        absmax = jnp.maximum(absmax, max_slots[w])
    max_out[...] = absmax
    inverse[...] = grid_levels / (absmax + epsilon)
    spread[...] = (absmax + epsilon) / (grid_levels * workers)

    def encode(target, rows_at, put):
        for i in range(blocks_each):
            block = target * blocks_each + i
            values = delta(block, rows_at) * column_of(inverse[pl.ds(block, 1), :])[rows_at]
            nearest = (values + SHIFT) - SHIFT
            rest = smooth_rest(smooth_rest(values - nearest))
            put(i, (nearest + rest).astype(jnp.bfloat16))

    def far_first(turn):
        return 1 + lax.rem(turn - 1 + (workers // 2 - 1), workers - 1)

    def enc_copy(part, turn):
        step = far_first(turn)
        return pltpu.make_async_remote_copy(
            src_ref=encoded.at[part, peer(step)], dst_ref=arrived.at[part, me],
            send_sem=enc_send.at[part, step], recv_sem=enc_recv.at[part, step],
            device_id={"replica": peer(step)}, device_id_type=MESH,
        )

    for part in range(parts):
        rows_at = slice(part * half, (part + 1) * half)

        @pl.loop(1, workers)
        def _(turn):
            target = peer(far_first(turn))

            def put(i, value):
                encoded[part, target, :, i * BLOCK : (i + 1) * BLOCK] = value

            encode(target, rows_at, put)

            @pl.when(turn > 1)
            def _():
                enc_copy(part, turn - 1).start()

        def put_own(i, value):
            total[rows_at, i * BLOCK : (i + 1) * BLOCK] = value.astype(jnp.float32)

        encode(me, rows_at, put_own)
        enc_copy(part, workers - 1).start()

    pairs = workers // 2
    low = lax.rem(me, 2)
    high = me // 2
    partner = me + 1 - 2 * low

    def place(worker, part):
        return grad_out.at[
            part * half : (part + 1) * half, pl.ds(pl.multiple_of(worker * width, BLOCK), width)
        ]

    def ring_origin(step):
        return lax.rem(high + pairs - step, pairs) * 2 + low

    def gat_copy(part, step):
        return pltpu.make_async_remote_copy(
            src_ref=share.at[part], dst_ref=place(me, part),
            send_sem=gat_send.at[part, step], recv_sem=gat_recv.at[part, step],
            device_id={"replica": lax.rem(high + step, pairs) * 2 + low}, device_id_type=MESH,
        )

    def own_forward(part):
        return pltpu.make_async_remote_copy(
            src_ref=share.at[part], dst_ref=place(me, part),
            send_sem=fwd_send.at[part, 0], recv_sem=fwd_recv.at[part, 0],
            device_id={"replica": partner}, device_id_type=MESH,
        )

    def forward(part, step):
        return pltpu.make_async_remote_copy(
            src_ref=place(ring_origin(step), part), dst_ref=place(ring_origin(step), part),
            send_sem=fwd_send.at[part, step], recv_sem=fwd_recv.at[part, step],
            device_id={"replica": partner}, device_id_type=MESH,
        )

    def own_copy(part):
        return pltpu.make_async_copy(share.at[part], place(me, part), own_sem.at[part])

    def sq_copy(step):
        return pltpu.make_async_remote_copy(
            src_ref=squares.at[me], dst_ref=squares.at[me],
            send_sem=sq_send.at[step], recv_sem=sq_recv.at[step],
            device_id={"replica": peer(step)}, device_id_type=MESH,
        )

    square = jnp.zeros((8, BLOCK), jnp.float32)
    for part in range(parts):
        rows_at = slice(part * half, (part + 1) * half)

        @pl.loop(1, workers)
        def _(turn):
            enc_copy(part, turn).wait()
            total[rows_at, :] += arrived[part, origin(far_first(turn))].astype(jnp.float32)

        for i in range(blocks_each):
            block = me * blocks_each + i
            at = slice(i * BLOCK, (i + 1) * BLOCK)
            value = total[rows_at, at] * column_of(spread[pl.ds(block, 1), :])[rows_at]
            share[part, :, at] = value.astype(jnp.bfloat16)
            square = square + jnp.sum((value * value).reshape(half // 8, 8, BLOCK), axis=0)

        if part == parts - 1:
            squares[me] = jnp.broadcast_to(jnp.sum(square, axis=0, keepdims=True), (8, BLOCK))

            @pl.loop(1, workers)
            def _(step):
                sq_copy(step).start()

        own_forward(part).start()

        @pl.loop(1, pairs)
        def _(step):
            gat_copy(part, step).start()

        own_copy(part).start()

    for part in range(parts):

        @pl.loop(1, pairs)
        def _(step):
            gat_copy(part, step).wait_recv()
            forward(part, step).start()

    @pl.loop(1, workers)
    def _(step):
        sq_copy(step).wait()

    part_sum = squares[0]
    for w in range(1, workers):
        part_sum = part_sum + squares[w]
    shard_squares[my_shard] = part_sum

    def ss_copy(step):
        return pltpu.make_async_remote_copy(
            src_ref=shard_squares.at[my_shard], dst_ref=shard_squares.at[my_shard],
            send_sem=ss_send.at[step], recv_sem=ss_recv.at[step],
            device_id={"shard": lax.rem(my_shard + step, shards)}, device_id_type=MESH,
        )

    @pl.loop(1, shards)
    def _(step):
        ss_copy(step).start()

    @pl.loop(1, shards)
    def _(step):
        ss_copy(step).wait()

    part_sum = shard_squares[0]
    for s in range(1, shards):
        part_sum = part_sum + shard_squares[s]
    mean = jnp.sum(part_sum, axis=1, keepdims=True) / entry_count
    root_mean = jnp.sqrt(mean + epsilon)
    factor_out[...] = jnp.broadcast_to(jnp.minimum(1.0, clip_level / root_mean), factor_out.shape)

    for part in range(parts):
        own_copy(part).wait()

        @pl.loop(1, pairs)
        def _(step):
            gat_copy(part, step).wait_send()
            forward(part, step).wait()

        own_forward(part).wait()

    momentum_copy.wait()


def exchange(outer_params, local_params, momentum):
    workers = lax.axis_size("replica")
    shards = lax.axis_size("shard")
    rows, cols = outer_params.shape
    blocks = cols // BLOCK
    width = cols // workers
    parts = 2
    half = rows // parts
    dma = pltpu.SemaphoreType.DMA
    vmem = pl.BlockSpec(memory_space=pltpu.VMEM)
    hbm = pl.BlockSpec(memory_space=pltpu.HBM)
    anywhere = pl.BlockSpec(memory_space=pl.ANY)
    return pl.pallas_call(
        functools.partial(exchange_kernel, workers, shards, rows * shards * cols),
        out_shape=(
            jax.ShapeDtypeStruct((rows, cols), jnp.bfloat16),
            jax.ShapeDtypeStruct((rows, cols), jnp.float32),
            jax.ShapeDtypeStruct((blocks, rows), jnp.float32),
            jax.ShapeDtypeStruct((8, BLOCK), jnp.float32),
        ),
        in_specs=[hbm, hbm, hbm],
        out_specs=(anywhere, anywhere, vmem, vmem),
        scratch_shapes=[
            pltpu.VMEM((rows, cols), jnp.float32),
            pltpu.VMEM((rows, cols), jnp.bfloat16),
            pltpu.VMEM((workers, blocks, rows), jnp.float32),
            pltpu.VMEM((blocks, rows), jnp.float32),
            pltpu.VMEM((blocks, rows), jnp.float32),
            pltpu.VMEM((parts, workers, half, width), jnp.bfloat16),
            pltpu.VMEM((parts, workers, half, width), jnp.bfloat16),
            pltpu.VMEM((rows, width), jnp.float32),
            pltpu.VMEM((parts, half, width), jnp.bfloat16),
            pltpu.VMEM((workers, 8, BLOCK), jnp.float32),
            pltpu.VMEM((shards, 8, BLOCK), jnp.float32),
            dma((2, 4)),
            dma((workers,)), dma((workers,)),
            dma((parts, workers)), dma((parts, workers)),
            dma((workers,)), dma((workers,)),
            dma((shards,)), dma((shards,)),
            dma((parts, workers // 2)), dma((parts, workers // 2)),
            dma((parts, workers // 2)), dma((parts, workers // 2)),
            dma((parts,)), dma(()),
        ],
        compiler_params=pltpu.CompilerParams(
            collective_id=0, has_side_effects=True, vmem_limit_bytes=16 * 2**20
        ),
        cost_estimate=pl.CostEstimate(
            flops=50 * rows * cols, bytes_accessed=8 * rows * cols * 4, transcendentals=0
        ),
    )(*(pltpu.with_memory_space_constraint(x, pltpu.HBM) for x in (outer_params, local_params, momentum)))


def per_device(outer_params, local_params, momentum):
    gradient, momentum, absmax, factor = exchange(outer_params, local_params, momentum)
    clipped = factor[0, 0] * gradient.astype(jnp.float32)
    momentum_next = outer_decay * momentum + clipped
    params_next = outer_params - outer_rate * (clipped + outer_decay * momentum_next)
    return (params_next, momentum_next, absmax)


def solution(mesh):
    return jax.shard_map(
        per_device,
        mesh=mesh,
        in_specs=(P("shard", None), P("replica", "shard", None), P("shard", None)),
        out_specs=(P("shard", None), P("shard", None), P(None, "shard")),
        check_vma=False,
    )
```

```python
import functools

import jax
import jax.numpy as jnp
from jax import lax
from jax.experimental import pallas as pl
from jax.experimental.pallas import tpu as pltpu
from jax.sharding import PartitionSpec as P

BLOCK = 128
MESH = pl.DeviceIdType.MESH

epsilon = 1e-06
clip_level = 0.5
outer_rate = 0.7
outer_decay = 0.9
grid_levels = 7.0

SMOOTH = (6.57973588, -12.98785441, 12.20756634, -6.687892761, 2.368806331, -0.5120006377)
SHIFT = 1.5 * 2.0**23


def smooth_rest(rest):
    square = rest * rest
    value = SMOOTH[-1]
    for coefficient in SMOOTH[-2::-1]:
        value = value * square + coefficient
    return rest * square * value


def column_of(row):
    return jnp.broadcast_to(row, (BLOCK, row.shape[1])).T


def exchange_kernel(
    workers, shards, entry_count,
    outer_hbm, local_hbm, momentum_hbm, grad_out, momentum_out, max_out, factor_out,
    outer_v, local_v, max_slots, inverse, spread, encoded, arrived, total, share, squares, shard_squares,
    load_sem, max_send, max_recv, enc_send, enc_recv, sq_send, sq_recv, ss_send, ss_recv, gat_send, gat_recv, fwd_send, fwd_recv, own_sem, momentum_sem,
):
    me = lax.axis_index("replica")
    my_shard = lax.axis_index("shard")
    rows, cols = outer_v.shape
    blocks = cols // BLOCK
    width = cols // workers
    blocks_each = width // BLOCK
    parts, half = share.shape[:2]
    pieces = load_sem.shape[1]
    piece = cols // pieces

    def peer(step):
        return lax.rem(me + step, workers)

    def origin(step):
        return lax.rem(me + workers - step, workers)

    def loads(i):
        part = pl.ds(i * piece, piece)
        return (
            pltpu.make_async_copy(outer_hbm.at[:, part], outer_v.at[:, part], load_sem.at[0, i]),
            pltpu.make_async_copy(local_hbm.at[0, :, part], local_v.at[:, part], load_sem.at[1, i]),
        )

    for i in range(pieces):
        for copy in loads(i):
            copy.start()
    momentum_copy = pltpu.make_async_copy(momentum_hbm, momentum_out, momentum_sem)

    barrier = pltpu.get_barrier_semaphore()

    @pl.loop(1, workers)
    def _(step):
        pl.semaphore_signal(barrier, inc=1, device_id={"replica": peer(step)}, device_id_type=MESH)

    @pl.loop(1, shards)
    def _(step):
        pl.semaphore_signal(
            barrier, inc=1, device_id={"shard": lax.rem(my_shard + step, shards)}, device_id_type=MESH
        )

    def delta(block, rows_at=slice(None)):
        at = pl.ds(pl.multiple_of(block * BLOCK, BLOCK), BLOCK)
        return outer_v[rows_at, at] - local_v[rows_at, at].astype(jnp.float32)

    per_piece = piece // BLOCK

    def max_copy(i, step):
        mine = max_slots.at[me, pl.ds(i * per_piece, per_piece)]
        return pltpu.make_async_remote_copy(
            src_ref=mine, dst_ref=mine,
            send_sem=max_send.at[i, step], recv_sem=max_recv.at[i, step],
            device_id={"replica": peer(step)}, device_id_type=MESH,
        )

    together = 4
    for i in range(pieces):
        for copy in loads(i):
            copy.wait()

        @pl.loop(0, per_piece // together)
        def _(group):
            for j in range(together):
                block = i * per_piece + group * together + j
                max_slots[me, pl.ds(block, 1), :] = jnp.max(jnp.abs(delta(block)).T, axis=0, keepdims=True)

        if i == 0:
            pl.semaphore_wait(barrier, workers + shards - 2)

        @pl.loop(1, workers)
        def _(step):
            max_copy(i, step).start()

    momentum_copy.start()
    for i in range(pieces):

        @pl.loop(1, workers)
        def _(step):
            max_copy(i, step).wait()

    absmax = max_slots[0]
    for w in range(1, workers):
        absmax = jnp.maximum(absmax, max_slots[w])
    max_out[...] = absmax
    inverse[...] = grid_levels / (absmax + epsilon)
    spread[...] = (absmax + epsilon) / (grid_levels * workers)

    def encode(target, rows_at, put):
        for i in range(blocks_each):
            block = target * blocks_each + i
            values = delta(block, rows_at) * column_of(inverse[pl.ds(block, 1), :][:, rows_at])
            nearest = (values + SHIFT) - SHIFT
            rest = smooth_rest(smooth_rest(values - nearest))
            put(i, (nearest + rest).astype(jnp.bfloat16))

    def far_first(turn):
        return 1 + lax.rem(turn - 1 + (workers // 2 - 1), workers - 1)

    def enc_copy(part, turn):
        step = far_first(turn)
        return pltpu.make_async_remote_copy(
            src_ref=encoded.at[part, peer(step)], dst_ref=arrived.at[part, me],
            send_sem=enc_send.at[part, step], recv_sem=enc_recv.at[part, step],
            device_id={"replica": peer(step)}, device_id_type=MESH,
        )

    for part in range(parts):
        rows_at = slice(part * half, (part + 1) * half)

        @pl.loop(1, workers)
        def _(turn):
            target = peer(far_first(turn))

            def put(i, value):
                encoded[part, target, :, i * BLOCK : (i + 1) * BLOCK] = value

            encode(target, rows_at, put)

            @pl.when(turn > 1)
            def _():
                enc_copy(part, turn - 1).start()

        def put_own(i, value):
            total[rows_at, i * BLOCK : (i + 1) * BLOCK] = value.astype(jnp.float32)

        encode(me, rows_at, put_own)
        enc_copy(part, workers - 1).start()

    pairs = workers // 2
    low = lax.rem(me, 2)
    high = me // 2
    partner = me + 1 - 2 * low

    def place(worker, part):
        return grad_out.at[
            part * half : (part + 1) * half, pl.ds(pl.multiple_of(worker * width, BLOCK), width)
        ]

    def ring_origin(step):
        return lax.rem(high + pairs - step, pairs) * 2 + low

    def gat_copy(part, step):
        return pltpu.make_async_remote_copy(
            src_ref=share.at[part], dst_ref=place(me, part),
            send_sem=gat_send.at[part, step], recv_sem=gat_recv.at[part, step],
            device_id={"replica": lax.rem(high + step, pairs) * 2 + low}, device_id_type=MESH,
        )

    def own_forward(part):
        return pltpu.make_async_remote_copy(
            src_ref=share.at[part], dst_ref=place(me, part),
            send_sem=fwd_send.at[part, 0], recv_sem=fwd_recv.at[part, 0],
            device_id={"replica": partner}, device_id_type=MESH,
        )

    def forward(part, step):
        return pltpu.make_async_remote_copy(
            src_ref=place(ring_origin(step), part), dst_ref=place(ring_origin(step), part),
            send_sem=fwd_send.at[part, step], recv_sem=fwd_recv.at[part, step],
            device_id={"replica": partner}, device_id_type=MESH,
        )

    def own_copy(part):
        return pltpu.make_async_copy(share.at[part], place(me, part), own_sem.at[part])

    def sq_copy(step):
        return pltpu.make_async_remote_copy(
            src_ref=squares.at[me], dst_ref=squares.at[me],
            send_sem=sq_send.at[step], recv_sem=sq_recv.at[step],
            device_id={"replica": peer(step)}, device_id_type=MESH,
        )

    square = jnp.zeros((8, BLOCK), jnp.float32)
    for part in range(parts):
        rows_at = slice(part * half, (part + 1) * half)

        @pl.loop(1, workers)
        def _(turn):
            enc_copy(part, turn).wait()
            total[rows_at, :] += arrived[part, origin(far_first(turn))].astype(jnp.float32)

        for i in range(blocks_each):
            block = me * blocks_each + i
            at = slice(i * BLOCK, (i + 1) * BLOCK)
            value = total[rows_at, at] * column_of(spread[pl.ds(block, 1), :][:, rows_at])
            share[part, :, at] = value.astype(jnp.bfloat16)
            square = square + jnp.sum((value * value).reshape(half // 8, 8, BLOCK), axis=0)

        if part == parts - 1:
            squares[me] = jnp.broadcast_to(jnp.sum(square, axis=0, keepdims=True), (8, BLOCK))

            @pl.loop(1, workers)
            def _(step):
                sq_copy(step).start()

        own_forward(part).start()

        @pl.loop(1, pairs)
        def _(step):
            gat_copy(part, step).start()

        own_copy(part).start()

    for part in range(parts):

        @pl.loop(1, pairs)
        def _(step):
            gat_copy(part, step).wait_recv()
            forward(part, step).start()

    @pl.loop(1, workers)
    def _(step):
        sq_copy(step).wait()

    part_sum = squares[0]
    for w in range(1, workers):
        part_sum = part_sum + squares[w]
    shard_squares[my_shard] = part_sum

    def ss_copy(step):
        return pltpu.make_async_remote_copy(
            src_ref=shard_squares.at[my_shard], dst_ref=shard_squares.at[my_shard],
            send_sem=ss_send.at[step], recv_sem=ss_recv.at[step],
            device_id={"shard": lax.rem(my_shard + step, shards)}, device_id_type=MESH,
        )

    @pl.loop(1, shards)
    def _(step):
        ss_copy(step).start()

    @pl.loop(1, shards)
    def _(step):
        ss_copy(step).wait()

    part_sum = shard_squares[0]
    for s in range(1, shards):
        part_sum = part_sum + shard_squares[s]
    mean = jnp.sum(part_sum, axis=1, keepdims=True) / entry_count
    root_mean = jnp.sqrt(mean + epsilon)
    factor_out[...] = jnp.broadcast_to(jnp.minimum(1.0, clip_level / root_mean), factor_out.shape)

    for part in range(parts):
        own_copy(part).wait()

        @pl.loop(1, pairs)
        def _(step):
            gat_copy(part, step).wait_send()
            forward(part, step).wait()

        own_forward(part).wait()

    momentum_copy.wait()


def exchange(outer_params, local_params, momentum):
    workers = lax.axis_size("replica")
    shards = lax.axis_size("shard")
    rows, cols = outer_params.shape
    blocks = cols // BLOCK
    width = cols // workers
    parts = 2
    half = rows // parts
    dma = pltpu.SemaphoreType.DMA
    vmem = pl.BlockSpec(memory_space=pltpu.VMEM)
    hbm = pl.BlockSpec(memory_space=pltpu.HBM)
    anywhere = pl.BlockSpec(memory_space=pl.ANY)
    return pl.pallas_call(
        functools.partial(exchange_kernel, workers, shards, rows * shards * cols),
        out_shape=(
            jax.ShapeDtypeStruct((rows, cols), jnp.bfloat16),
            jax.ShapeDtypeStruct((rows, cols), jnp.float32),
            jax.ShapeDtypeStruct((blocks, rows), jnp.float32),
            jax.ShapeDtypeStruct((8, BLOCK), jnp.float32),
        ),
        in_specs=[hbm, hbm, hbm],
        out_specs=(anywhere, anywhere, vmem, vmem),
        scratch_shapes=[
            pltpu.VMEM((rows, cols), jnp.float32),
            pltpu.VMEM((rows, cols), jnp.bfloat16),
            pltpu.VMEM((workers, blocks, rows), jnp.float32),
            pltpu.VMEM((blocks, rows), jnp.float32),
            pltpu.VMEM((blocks, rows), jnp.float32),
            pltpu.VMEM((parts, workers, half, width), jnp.bfloat16),
            pltpu.VMEM((parts, workers, half, width), jnp.bfloat16),
            pltpu.VMEM((rows, width), jnp.float32),
            pltpu.VMEM((parts, half, width), jnp.bfloat16),
            pltpu.VMEM((workers, 8, BLOCK), jnp.float32),
            pltpu.VMEM((shards, 8, BLOCK), jnp.float32),
            dma((2, 4)),
            dma((4, workers)), dma((4, workers)),
            dma((parts, workers)), dma((parts, workers)),
            dma((workers,)), dma((workers,)),
            dma((shards,)), dma((shards,)),
            dma((parts, workers // 2)), dma((parts, workers // 2)),
            dma((parts, workers // 2)), dma((parts, workers // 2)),
            dma((parts,)), dma(()),
        ],
        compiler_params=pltpu.CompilerParams(
            collective_id=0, has_side_effects=True, vmem_limit_bytes=16 * 2**20
        ),
        cost_estimate=pl.CostEstimate(
            flops=50 * rows * cols, bytes_accessed=8 * rows * cols * 4, transcendentals=0
        ),
    )(*(pltpu.with_memory_space_constraint(x, pltpu.HBM) for x in (outer_params, local_params, momentum)))


def per_device(outer_params, local_params, momentum):
    gradient, momentum, absmax, factor = exchange(outer_params, local_params, momentum)
    clipped = factor[0, 0] * gradient.astype(jnp.float32)
    momentum_next = outer_decay * momentum + clipped
    params_next = outer_params - outer_rate * (clipped + outer_decay * momentum_next)
    return (params_next, momentum_next, absmax)


def solution(mesh):
    return jax.shard_map(
        per_device,
        mesh=mesh,
        in_specs=(P("shard", None), P("replica", "shard", None), P("shard", None)),
        out_specs=(P("shard", None), P("shard", None), P(None, "shard")),
        check_vma=False,
    )
```

```python
import functools

import jax
import jax.numpy as jnp
from jax import lax
from jax.experimental import pallas as pl
from jax.experimental.pallas import tpu as pltpu
from jax.sharding import PartitionSpec as P

BLOCK = 128
MESH = pl.DeviceIdType.MESH

epsilon = 1e-06
clip_level = 0.5
outer_rate = 0.7
outer_decay = 0.9
grid_levels = 7.0

SMOOTH = (6.57973588, -12.98785441, 12.20756634, -6.687892761, 2.368806331, -0.5120006377)
SHIFT = 1.5 * 2.0**23


def smooth_rest(rest):
    square = rest * rest
    value = SMOOTH[-1]
    for coefficient in SMOOTH[-2::-1]:
        value = value * square + coefficient
    return rest * square * value


def column_of(row):
    return jnp.broadcast_to(row, (BLOCK, row.shape[1])).T


def exchange_kernel(
    workers, shards, entry_count,
    outer_hbm, local_hbm, momentum_hbm, grad_out, momentum_out, max_out, factor_out,
    outer_v, local_v, max_slots, inverse, spread, encoded, arrived, total, share, squares, shard_squares,
    load_sem, max_send, max_recv, enc_send, enc_recv, sq_send, sq_recv, ss_send, ss_recv, gat_send, gat_recv, fwd_send, fwd_recv, own_sem, momentum_sem,
):
    me = lax.axis_index("replica")
    my_shard = lax.axis_index("shard")
    rows, cols = outer_v.shape
    blocks = cols // BLOCK
    width = cols // workers
    blocks_each = width // BLOCK
    parts, half = share.shape[:2]
    pieces = load_sem.shape[1]
    piece = cols // pieces

    def peer(step):
        return lax.rem(me + step, workers)

    def origin(step):
        return lax.rem(me + workers - step, workers)

    def loads(i):
        part = pl.ds(i * piece, piece)
        return (
            pltpu.make_async_copy(outer_hbm.at[:, part], outer_v.at[:, part], load_sem.at[0, i]),
            pltpu.make_async_copy(local_hbm.at[0, :, part], local_v.at[:, part], load_sem.at[1, i]),
        )

    for i in range(pieces):
        for copy in loads(i):
            copy.start()
    momentum_copy = pltpu.make_async_copy(momentum_hbm, momentum_out, momentum_sem)

    barrier = pltpu.get_barrier_semaphore()

    @pl.loop(1, workers)
    def _(step):
        pl.semaphore_signal(barrier, inc=1, device_id={"replica": peer(step)}, device_id_type=MESH)

    @pl.loop(1, shards)
    def _(step):
        pl.semaphore_signal(
            barrier, inc=1, device_id={"shard": lax.rem(my_shard + step, shards)}, device_id_type=MESH
        )

    def delta(block, rows_at=slice(None)):
        at = pl.ds(pl.multiple_of(block * BLOCK, BLOCK), BLOCK)
        return outer_v[rows_at, at] - local_v[rows_at, at].astype(jnp.float32)

    per_piece = piece // BLOCK

    def max_copy(i, step):
        mine = max_slots.at[me, pl.ds(i * per_piece, per_piece)]
        return pltpu.make_async_remote_copy(
            src_ref=mine, dst_ref=mine,
            send_sem=max_send.at[i, step], recv_sem=max_recv.at[i, step],
            device_id={"replica": peer(step)}, device_id_type=MESH,
        )

    together = 4
    for i in range(pieces):
        for copy in loads(i):
            copy.wait()

        @pl.loop(0, per_piece // together)
        def _(group):
            for j in range(together):
                block = i * per_piece + group * together + j
                max_slots[me, pl.ds(block, 1), :] = jnp.max(jnp.abs(delta(block)).T, axis=0, keepdims=True)

        if i == 0:
            pl.semaphore_wait(barrier, workers + shards - 2)

        @pl.loop(1, workers)
        def _(step):
            max_copy(i, step).start()

    momentum_copy.start()
    for i in range(pieces):

        @pl.loop(1, workers)
        def _(step):
            max_copy(i, step).wait()

    absmax = max_slots[0]
    for w in range(1, workers):
        absmax = jnp.maximum(absmax, max_slots[w])
    max_out[...] = absmax
    inverse[...] = grid_levels / (absmax + epsilon)
    spread[...] = (absmax + epsilon) / (grid_levels * workers)

    def encode(target, rows_at, put):
        for i in range(blocks_each):
            block = target * blocks_each + i
            values = delta(block, rows_at) * column_of(inverse[pl.ds(block, 1), :][:, rows_at])
            nearest = (values + SHIFT) - SHIFT
            rest = smooth_rest(smooth_rest(values - nearest))
            put(i, (nearest + rest).astype(jnp.bfloat16))

    def far_first(turn):
        return 1 + lax.rem(turn - 1 + (workers // 2 - 1), workers - 1)

    def enc_copy(part, turn):
        step = far_first(turn)
        return pltpu.make_async_remote_copy(
            src_ref=encoded.at[part, peer(step)], dst_ref=arrived.at[part, me],
            send_sem=enc_send.at[part, step], recv_sem=enc_recv.at[part, step],
            device_id={"replica": peer(step)}, device_id_type=MESH,
        )

    for part in range(parts):
        rows_at = slice(part * half, (part + 1) * half)

        @pl.loop(1, workers)
        def _(turn):
            target = peer(far_first(turn))

            def put(i, value):
                encoded[part, target, :, i * BLOCK : (i + 1) * BLOCK] = value

            encode(target, rows_at, put)

            @pl.when(turn > 1)
            def _():
                enc_copy(part, turn - 1).start()

        def put_own(i, value):
            total[rows_at, i * BLOCK : (i + 1) * BLOCK] = value.astype(jnp.float32)

        encode(me, rows_at, put_own)
        enc_copy(part, workers - 1).start()

    pairs = workers // 2
    low = lax.rem(me, 2)
    high = me // 2
    partner = me + 1 - 2 * low

    def place(worker, part):
        return grad_out.at[
            part * half : (part + 1) * half, pl.ds(pl.multiple_of(worker * width, BLOCK), width)
        ]

    def ring_origin(step):
        return lax.rem(high + pairs - step, pairs) * 2 + low

    def gat_copy(part, step):
        return pltpu.make_async_remote_copy(
            src_ref=share.at[part], dst_ref=place(me, part),
            send_sem=gat_send.at[part, step], recv_sem=gat_recv.at[part, step],
            device_id={"replica": lax.rem(high + step, pairs) * 2 + low}, device_id_type=MESH,
        )

    def own_forward(part):
        return pltpu.make_async_remote_copy(
            src_ref=share.at[part], dst_ref=place(me, part),
            send_sem=fwd_send.at[part, 0], recv_sem=fwd_recv.at[part, 0],
            device_id={"replica": partner}, device_id_type=MESH,
        )

    def forward(part, step):
        return pltpu.make_async_remote_copy(
            src_ref=place(ring_origin(step), part), dst_ref=place(ring_origin(step), part),
            send_sem=fwd_send.at[part, step], recv_sem=fwd_recv.at[part, step],
            device_id={"replica": partner}, device_id_type=MESH,
        )

    def own_copy(part):
        return pltpu.make_async_copy(share.at[part], place(me, part), own_sem.at[part])

    def sq_copy(step):
        return pltpu.make_async_remote_copy(
            src_ref=squares.at[me], dst_ref=squares.at[me],
            send_sem=sq_send.at[step], recv_sem=sq_recv.at[step],
            device_id={"replica": peer(step)}, device_id_type=MESH,
        )

    square = jnp.zeros((8, BLOCK), jnp.float32)
    for part in range(parts):
        rows_at = slice(part * half, (part + 1) * half)

        @pl.loop(1, workers)
        def _(turn):
            enc_copy(part, turn).wait()
            total[rows_at, :] += arrived[part, origin(far_first(turn))].astype(jnp.float32)

        for i in range(blocks_each):
            block = me * blocks_each + i
            at = slice(i * BLOCK, (i + 1) * BLOCK)
            value = total[rows_at, at] * column_of(spread[pl.ds(block, 1), :][:, rows_at])
            share[part, :, at] = value.astype(jnp.bfloat16)
            square = square + jnp.sum((value * value).reshape(half // 8, 8, BLOCK), axis=0)

        if part == parts - 1:
            squares[me] = jnp.broadcast_to(jnp.sum(square, axis=0, keepdims=True), (8, BLOCK))

            @pl.loop(1, workers)
            def _(step):
                sq_copy(step).start()

        own_forward(part).start()

        @pl.loop(1, pairs)
        def _(step):
            gat_copy(part, step).start()

        own_copy(part).start()

    for part in range(parts):

        @pl.loop(1, pairs)
        def _(step):
            gat_copy(part, step).wait_recv()
            forward(part, step).start()

    @pl.loop(1, workers)
    def _(step):
        sq_copy(step).wait()

    part_sum = squares[0]
    for w in range(1, workers):
        part_sum = part_sum + squares[w]
    shard_squares[my_shard] = part_sum

    def ss_copy(step):
        return pltpu.make_async_remote_copy(
            src_ref=shard_squares.at[my_shard], dst_ref=shard_squares.at[my_shard],
            send_sem=ss_send.at[step], recv_sem=ss_recv.at[step],
            device_id={"shard": lax.rem(my_shard + step, shards)}, device_id_type=MESH,
        )

    @pl.loop(1, shards)
    def _(step):
        ss_copy(step).start()

    @pl.loop(1, shards)
    def _(step):
        ss_copy(step).wait()

    part_sum = shard_squares[0]
    for s in range(1, shards):
        part_sum = part_sum + shard_squares[s]
    mean = jnp.sum(part_sum, axis=1, keepdims=True) / entry_count
    root_mean = jnp.sqrt(mean + epsilon)
    factor_out[...] = jnp.broadcast_to(jnp.minimum(1.0, clip_level / root_mean), factor_out.shape)

    for part in range(parts):
        own_copy(part).wait()

        @pl.loop(1, pairs)
        def _(step):
            gat_copy(part, step).wait_send()
            forward(part, step).wait()

        own_forward(part).wait()

    momentum_copy.wait()


def exchange(outer_params, local_params, momentum):
    workers = lax.axis_size("replica")
    shards = lax.axis_size("shard")
    rows, cols = outer_params.shape
    blocks = cols // BLOCK
    width = cols // workers
    parts = 2
    half = rows // parts
    dma = pltpu.SemaphoreType.DMA
    vmem = pl.BlockSpec(memory_space=pltpu.VMEM)
    hbm = pl.BlockSpec(memory_space=pltpu.HBM)
    anywhere = pl.BlockSpec(memory_space=pl.ANY)
    return pl.pallas_call(
        functools.partial(exchange_kernel, workers, shards, rows * shards * cols),
        out_shape=(
            jax.ShapeDtypeStruct((rows, cols), jnp.bfloat16),
            jax.ShapeDtypeStruct((rows, cols), jnp.float32),
            jax.ShapeDtypeStruct((blocks, rows), jnp.float32),
            jax.ShapeDtypeStruct((8, BLOCK), jnp.float32),
        ),
        in_specs=[hbm, hbm, hbm],
        out_specs=(anywhere, anywhere, vmem, vmem),
        scratch_shapes=[
            pltpu.VMEM((rows, cols), jnp.float32),
            pltpu.VMEM((rows, cols), jnp.bfloat16),
            pltpu.VMEM((workers, blocks, rows), jnp.float32),
            pltpu.VMEM((blocks, rows), jnp.float32),
            pltpu.VMEM((blocks, rows), jnp.float32),
            pltpu.VMEM((parts, workers, half, width), jnp.bfloat16),
            pltpu.VMEM((parts, workers, half, width), jnp.bfloat16),
            pltpu.VMEM((rows, width), jnp.float32),
            pltpu.VMEM((parts, half, width), jnp.bfloat16),
            pltpu.VMEM((workers, 8, BLOCK), jnp.float32),
            pltpu.VMEM((shards, 8, BLOCK), jnp.float32),
            dma((2, 4)),
            dma((4, workers)), dma((4, workers)),
            dma((parts, workers)), dma((parts, workers)),
            dma((workers,)), dma((workers,)),
            dma((shards,)), dma((shards,)),
            dma((parts, workers // 2)), dma((parts, workers // 2)),
            dma((parts, workers // 2)), dma((parts, workers // 2)),
            dma((parts,)), dma(()),
        ],
        compiler_params=pltpu.CompilerParams(
            collective_id=0, has_side_effects=True, vmem_limit_bytes=16 * 2**20
        ),
        cost_estimate=pl.CostEstimate(
            flops=50 * rows * cols, bytes_accessed=8 * rows * cols * 4, transcendentals=0
        ),
    )(*(pltpu.with_memory_space_constraint(x, pltpu.HBM) for x in (outer_params, local_params, momentum)))


def finish_kernel(
    factor_ref, outer_ref, gradient_ref, momentum_ref, max_ref, params_out, next_out, max_out,
    params_v, next_v, sem, max_sem,
):
    tiles = sem.shape[1]
    rows = outer_ref.shape[0] // tiles
    maxima = pltpu.make_async_copy(max_ref, max_out, max_sem)
    maxima.start()

    def stores(tile):
        at = pl.ds(tile * rows, rows)
        return (
            pltpu.make_async_copy(next_v.at[at], next_out.at[at], sem.at[0, tile]),
            pltpu.make_async_copy(params_v.at[at], params_out.at[at], sem.at[1, tile]),
        )

    factor = factor_ref[0:1, 0:1]

    @pl.loop(0, tiles)
    def _(tile):
        at = pl.ds(pl.multiple_of(tile * rows, rows), rows)
        clipped = factor * gradient_ref[at, :].astype(jnp.float32)
        momentum_next = outer_decay * momentum_ref[at, :] + clipped
        next_v[at, :] = momentum_next
        params_v[at, :] = outer_ref[at, :] - outer_rate * (clipped + outer_decay * momentum_next)
        for copy in stores(tile):
            copy.start()

    @pl.loop(0, tiles)
    def _(tile):
        for copy in stores(tile):
            copy.wait()

    maxima.wait()


def finish(factor, outer_params, gradient, momentum, absmax):
    rows, cols = outer_params.shape
    tiles = rows // 16
    vmem = pl.BlockSpec(memory_space=pltpu.VMEM)
    hbm = pl.BlockSpec(memory_space=pltpu.HBM)
    return pl.pallas_call(
        finish_kernel,
        out_shape=(
            pltpu.HBM((rows, cols), jnp.float32),
            pltpu.HBM((rows, cols), jnp.float32),
            pltpu.HBM(absmax.shape, jnp.float32),
        ),
        in_specs=[vmem] * 5,
        out_specs=(hbm, hbm, hbm),
        scratch_shapes=[
            pltpu.VMEM((rows, cols), jnp.float32),
            pltpu.VMEM((rows, cols), jnp.float32),
            pltpu.SemaphoreType.DMA((2, tiles)),
            pltpu.SemaphoreType.DMA(()),
        ],
        compiler_params=pltpu.CompilerParams(vmem_limit_bytes=16 * 2**20),
        cost_estimate=pl.CostEstimate(
            flops=6 * rows * cols, bytes_accessed=18 * rows * cols, transcendentals=0
        ),
    )(factor, outer_params, gradient, momentum, absmax)


def per_device(outer_params, local_params, momentum):
    gradient, momentum, absmax, factor = exchange(outer_params, local_params, momentum)
    return finish(factor, outer_params, gradient, momentum, absmax)


def solution(mesh):
    return jax.shard_map(
        per_device,
        mesh=mesh,
        in_specs=(P("shard", None), P("replica", "shard", None), P("shard", None)),
        out_specs=(P("shard", None), P("shard", None), P(None, "shard")),
        check_vma=False,
    )
```

```python
import functools

import jax
import jax.numpy as jnp
from jax import lax
from jax.experimental import pallas as pl
from jax.experimental.pallas import tpu as pltpu
from jax.sharding import PartitionSpec as P

BLOCK = 128
MESH = pl.DeviceIdType.MESH

epsilon = 1e-06
clip_level = 0.5
outer_rate = 0.7
outer_decay = 0.9
grid_levels = 7.0

SMOOTH = (6.57973588, -12.98785441, 12.20756634, -6.687892761, 2.368806331, -0.5120006377)
SHIFT = 1.5 * 2.0**23


def smooth_rest(rest):
    square = rest * rest
    value = SMOOTH[-1]
    for coefficient in SMOOTH[-2::-1]:
        value = value * square + coefficient
    return rest * square * value


def column_of(row):
    return jnp.broadcast_to(row, (BLOCK, row.shape[1])).T


def exchange_kernel(
    workers, shards, entry_count,
    outer_hbm, local_hbm, momentum_hbm, grad_out, momentum_out, max_out, factor_out,
    outer_v, local_v, max_slots, inverse, spread, encoded, arrived, total, share, squares, shard_squares,
    load_sem, max_send, max_recv, enc_send, enc_recv, sq_send, sq_recv, ss_send, ss_recv, gat_send, gat_recv, cross_send, cross_recv, relay_send, fwd_send, fwd_recv, own_sem, momentum_sem,
):
    me = lax.axis_index("replica")
    my_shard = lax.axis_index("shard")
    rows, cols = outer_v.shape
    blocks = cols // BLOCK
    width = cols // workers
    blocks_each = width // BLOCK
    parts, half = share.shape[:2]
    pieces = load_sem.shape[1]
    piece = cols // pieces

    def peer(step):
        return lax.rem(me + step, workers)

    def origin(step):
        return lax.rem(me + workers - step, workers)

    def loads(i):
        part = pl.ds(i * piece, piece)
        return (
            pltpu.make_async_copy(outer_hbm.at[:, part], outer_v.at[:, part], load_sem.at[0, i]),
            pltpu.make_async_copy(local_hbm.at[0, :, part], local_v.at[:, part], load_sem.at[1, i]),
        )

    for i in range(pieces):
        for copy in loads(i):
            copy.start()
    momentum_copy = pltpu.make_async_copy(momentum_hbm, momentum_out, momentum_sem)

    barrier = pltpu.get_barrier_semaphore()

    @pl.loop(1, workers)
    def _(step):
        pl.semaphore_signal(barrier, inc=1, device_id={"replica": peer(step)}, device_id_type=MESH)

    @pl.loop(1, shards)
    def _(step):
        pl.semaphore_signal(
            barrier, inc=1, device_id={"shard": lax.rem(my_shard + step, shards)}, device_id_type=MESH
        )

    def delta(block, rows_at=slice(None)):
        at = pl.ds(pl.multiple_of(block * BLOCK, BLOCK), BLOCK)
        return outer_v[rows_at, at] - local_v[rows_at, at].astype(jnp.float32)

    per_piece = piece // BLOCK

    def max_copy(i, step):
        mine = max_slots.at[me, pl.ds(i * per_piece, per_piece)]
        return pltpu.make_async_remote_copy(
            src_ref=mine, dst_ref=mine,
            send_sem=max_send.at[i, step], recv_sem=max_recv.at[i, step],
            device_id={"replica": peer(step)}, device_id_type=MESH,
        )

    together = 4
    for i in range(pieces):
        for copy in loads(i):
            copy.wait()

        @pl.loop(0, per_piece // together)
        def _(group):
            for j in range(together):
                block = i * per_piece + group * together + j
                max_slots[me, pl.ds(block, 1), :] = jnp.max(jnp.abs(delta(block)).T, axis=0, keepdims=True)

        if i == 0:
            pl.semaphore_wait(barrier, workers + shards - 2)

        @pl.loop(1, workers)
        def _(step):
            max_copy(i, step).start()

    momentum_copy.start()
    for i in range(pieces):

        @pl.loop(1, workers)
        def _(step):
            max_copy(i, step).wait()

    absmax = max_slots[0]
    for w in range(1, workers):
        absmax = jnp.maximum(absmax, max_slots[w])
    max_out[...] = absmax
    inverse[...] = grid_levels / (absmax + epsilon)
    spread[...] = (absmax + epsilon) / (grid_levels * workers)

    def encode(target, rows_at, put):
        for i in range(blocks_each):
            block = target * blocks_each + i
            values = delta(block, rows_at) * column_of(inverse[pl.ds(block, 1), :][:, rows_at])
            nearest = (values + SHIFT) - SHIFT
            rest = smooth_rest(smooth_rest(values - nearest))
            put(i, (nearest + rest).astype(jnp.bfloat16))

    def far_first(turn):
        return 1 + lax.rem(turn - 1 + (workers // 2 - 1), workers - 1)

    def enc_copy(part, turn):
        step = far_first(turn)
        return pltpu.make_async_remote_copy(
            src_ref=encoded.at[part, peer(step)], dst_ref=arrived.at[part, me],
            send_sem=enc_send.at[part, step], recv_sem=enc_recv.at[part, step],
            device_id={"replica": peer(step)}, device_id_type=MESH,
        )

    for part in range(parts):
        rows_at = slice(part * half, (part + 1) * half)

        @pl.loop(1, workers)
        def _(turn):
            target = peer(far_first(turn))

            def put(i, value):
                encoded[part, target, :, i * BLOCK : (i + 1) * BLOCK] = value

            encode(target, rows_at, put)

            @pl.when(turn > 1)
            def _():
                enc_copy(part, turn - 1).start()

        def put_own(i, value):
            total[rows_at, i * BLOCK : (i + 1) * BLOCK] = value.astype(jnp.float32)

        encode(me, rows_at, put_own)
        enc_copy(part, workers - 1).start()

    pairs = workers // 2
    low = lax.rem(me, 2)
    high = me // 2
    partner = me + 1 - 2 * low

    def place(worker, part):
        return grad_out.at[
            part * half : (part + 1) * half, pl.ds(pl.multiple_of(worker * width, BLOCK), width)
        ]

    span = pairs // 2
    upper = high // span
    base = upper * span
    spot = high - base
    is_gateway = spot == (span - 1) * (1 - upper)
    other_gateway = span - upper

    def near_first(turn):
        return turn + upper * (span - 1 - 2 * turn)

    def inner_origin(step):
        return base + lax.rem(spot + span - step, span)

    def cross_origin(j):
        return (1 - upper) * span + j

    def inner_copy(part, step):
        return pltpu.make_async_remote_copy(
            src_ref=share.at[part], dst_ref=place(me, part),
            send_sem=gat_send.at[part, step], recv_sem=gat_recv.at[part, step],
            device_id={"replica": (base + lax.rem(spot + step, span)) * 2 + low}, device_id_type=MESH,
        )

    def cross_copy(part):
        return pltpu.make_async_remote_copy(
            src_ref=share.at[part], dst_ref=place(me, part),
            send_sem=cross_send.at[part], recv_sem=cross_recv.at[part, spot],
            device_id={"replica": other_gateway * 2 + low}, device_id_type=MESH,
        )

    def relay(part, j, step):
        chunk = place(cross_origin(j) * 2 + low, part)
        return pltpu.make_async_remote_copy(
            src_ref=chunk, dst_ref=chunk,
            send_sem=relay_send.at[part, j, step], recv_sem=cross_recv.at[part, j],
            device_id={"replica": (base + lax.rem(spot + step, span)) * 2 + low}, device_id_type=MESH,
        )

    def own_forward(part):
        return pltpu.make_async_remote_copy(
            src_ref=share.at[part], dst_ref=place(me, part),
            send_sem=fwd_send.at[part, high], recv_sem=fwd_recv.at[part, high],
            device_id={"replica": partner}, device_id_type=MESH,
        )

    def forward(part, row):
        chunk = place(row * 2 + low, part)
        return pltpu.make_async_remote_copy(
            src_ref=chunk, dst_ref=chunk,
            send_sem=fwd_send.at[part, row], recv_sem=fwd_recv.at[part, row],
            device_id={"replica": partner}, device_id_type=MESH,
        )

    def take_cross(part, turn):
        j = near_first(turn)
        relay(part, j, 1).wait_recv()

        @pl.when(is_gateway)
        def _():
            @pl.loop(1, span)
            def _(step):
                relay(part, j, step).start()

        forward(part, cross_origin(j)).start()

    def own_copy(part):
        return pltpu.make_async_copy(share.at[part], place(me, part), own_sem.at[part])

    def sq_copy(step):
        return pltpu.make_async_remote_copy(
            src_ref=squares.at[me], dst_ref=squares.at[me],
            send_sem=sq_send.at[step], recv_sem=sq_recv.at[step],
            device_id={"replica": peer(step)}, device_id_type=MESH,
        )

    square = jnp.zeros((8, BLOCK), jnp.float32)
    for part in range(parts):
        rows_at = slice(part * half, (part + 1) * half)

        @pl.loop(1, workers)
        def _(turn):
            enc_copy(part, turn).wait()
            total[rows_at, :] += arrived[part, origin(far_first(turn))].astype(jnp.float32)

        for i in range(blocks_each):
            block = me * blocks_each + i
            at = slice(i * BLOCK, (i + 1) * BLOCK)
            value = total[rows_at, at] * column_of(spread[pl.ds(block, 1), :][:, rows_at])
            share[part, :, at] = value.astype(jnp.bfloat16)
            square = square + jnp.sum((value * value).reshape(half // 8, 8, BLOCK), axis=0)

        if part == parts - 1:
            squares[me] = jnp.broadcast_to(jnp.sum(square, axis=0, keepdims=True), (8, BLOCK))

            @pl.loop(1, workers)
            def _(step):
                sq_copy(step).start()

        cross_copy(part).start()
        own_forward(part).start()

        @pl.loop(1, span)
        def _(step):
            inner_copy(part, step).start()

        own_copy(part).start()

    for part in range(parts):

        take_cross(part, 0)

        @pl.loop(1, span)
        def _(step):
            inner_copy(part, step).wait_recv()
            forward(part, inner_origin(step)).start()

        @pl.loop(1, span)
        def _(turn):
            take_cross(part, turn)

    @pl.loop(1, workers)
    def _(step):
        sq_copy(step).wait()

    part_sum = squares[0]
    for w in range(1, workers):
        part_sum = part_sum + squares[w]
    shard_squares[my_shard] = part_sum

    def ss_copy(step):
        return pltpu.make_async_remote_copy(
            src_ref=shard_squares.at[my_shard], dst_ref=shard_squares.at[my_shard],
            send_sem=ss_send.at[step], recv_sem=ss_recv.at[step],
            device_id={"shard": lax.rem(my_shard + step, shards)}, device_id_type=MESH,
        )

    @pl.loop(1, shards)
    def _(step):
        ss_copy(step).start()

    @pl.loop(1, shards)
    def _(step):
        ss_copy(step).wait()

    part_sum = shard_squares[0]
    for s in range(1, shards):
        part_sum = part_sum + shard_squares[s]
    mean = jnp.sum(part_sum, axis=1, keepdims=True) / entry_count
    root_mean = jnp.sqrt(mean + epsilon)
    factor_out[...] = jnp.broadcast_to(jnp.minimum(1.0, clip_level / root_mean), factor_out.shape)

    for part in range(parts):
        own_copy(part).wait()

        cross_copy(part).wait_send()

        @pl.loop(1, span)
        def _(step):
            inner_copy(part, step).wait_send()

        @pl.when(is_gateway)
        def _():
            @pl.loop(0, span)
            def _(j):
                @pl.loop(1, span)
                def _(step):
                    relay(part, j, step).wait_send()

        @pl.loop(0, pairs)
        def _(row):
            forward(part, row).wait()

    momentum_copy.wait()


def exchange(outer_params, local_params, momentum):
    workers = lax.axis_size("replica")
    shards = lax.axis_size("shard")
    rows, cols = outer_params.shape
    blocks = cols // BLOCK
    width = cols // workers
    parts = 2
    half = rows // parts
    dma = pltpu.SemaphoreType.DMA
    vmem = pl.BlockSpec(memory_space=pltpu.VMEM)
    hbm = pl.BlockSpec(memory_space=pltpu.HBM)
    anywhere = pl.BlockSpec(memory_space=pl.ANY)
    return pl.pallas_call(
        functools.partial(exchange_kernel, workers, shards, rows * shards * cols),
        out_shape=(
            jax.ShapeDtypeStruct((rows, cols), jnp.bfloat16),
            jax.ShapeDtypeStruct((rows, cols), jnp.float32),
            jax.ShapeDtypeStruct((blocks, rows), jnp.float32),
            jax.ShapeDtypeStruct((8, BLOCK), jnp.float32),
        ),
        in_specs=[hbm, hbm, hbm],
        out_specs=(anywhere, anywhere, vmem, vmem),
        scratch_shapes=[
            pltpu.VMEM((rows, cols), jnp.float32),
            pltpu.VMEM((rows, cols), jnp.bfloat16),
            pltpu.VMEM((workers, blocks, rows), jnp.float32),
            pltpu.VMEM((blocks, rows), jnp.float32),
            pltpu.VMEM((blocks, rows), jnp.float32),
            pltpu.VMEM((parts, workers, half, width), jnp.bfloat16),
            pltpu.VMEM((parts, workers, half, width), jnp.bfloat16),
            pltpu.VMEM((rows, width), jnp.float32),
            pltpu.VMEM((parts, half, width), jnp.bfloat16),
            pltpu.VMEM((workers, 8, BLOCK), jnp.float32),
            pltpu.VMEM((shards, 8, BLOCK), jnp.float32),
            dma((2, 4)),
            dma((4, workers)), dma((4, workers)),
            dma((parts, workers)), dma((parts, workers)),
            dma((workers,)), dma((workers,)),
            dma((shards,)), dma((shards,)),
            dma((parts, workers // 4)), dma((parts, workers // 4)),
            dma((parts,)), dma((parts, workers // 4)), dma((parts, workers // 4, workers // 4)),
            dma((parts, workers // 2)), dma((parts, workers // 2)),
            dma((parts,)), dma(()),
        ],
        compiler_params=pltpu.CompilerParams(
            collective_id=0, has_side_effects=True, vmem_limit_bytes=16 * 2**20
        ),
        cost_estimate=pl.CostEstimate(
            flops=50 * rows * cols, bytes_accessed=8 * rows * cols * 4, transcendentals=0
        ),
    )(*(pltpu.with_memory_space_constraint(x, pltpu.HBM) for x in (outer_params, local_params, momentum)))


def finish_kernel(
    factor_ref, outer_ref, gradient_ref, momentum_ref, max_ref, params_out, next_out, max_out,
    params_v, next_v, sem, max_sem,
):
    tiles = sem.shape[1]
    rows = outer_ref.shape[0] // tiles
    maxima = pltpu.make_async_copy(max_ref, max_out, max_sem)
    maxima.start()

    def stores(tile):
        at = pl.ds(tile * rows, rows)
        return (
            pltpu.make_async_copy(next_v.at[at], next_out.at[at], sem.at[0, tile]),
            pltpu.make_async_copy(params_v.at[at], params_out.at[at], sem.at[1, tile]),
        )

    factor = factor_ref[0:1, 0:1]

    @pl.loop(0, tiles)
    def _(tile):
        at = pl.ds(pl.multiple_of(tile * rows, rows), rows)
        clipped = factor * gradient_ref[at, :].astype(jnp.float32)
        momentum_next = outer_decay * momentum_ref[at, :] + clipped
        next_v[at, :] = momentum_next
        params_v[at, :] = outer_ref[at, :] - outer_rate * (clipped + outer_decay * momentum_next)
        for copy in stores(tile):
            copy.start()

    @pl.loop(0, tiles)
    def _(tile):
        for copy in stores(tile):
            copy.wait()

    maxima.wait()


def finish(factor, outer_params, gradient, momentum, absmax):
    rows, cols = outer_params.shape
    tiles = rows // 16
    vmem = pl.BlockSpec(memory_space=pltpu.VMEM)
    hbm = pl.BlockSpec(memory_space=pltpu.HBM)
    return pl.pallas_call(
        finish_kernel,
        out_shape=(
            pltpu.HBM((rows, cols), jnp.float32),
            pltpu.HBM((rows, cols), jnp.float32),
            pltpu.HBM(absmax.shape, jnp.float32),
        ),
        in_specs=[vmem] * 5,
        out_specs=(hbm, hbm, hbm),
        scratch_shapes=[
            pltpu.VMEM((rows, cols), jnp.float32),
            pltpu.VMEM((rows, cols), jnp.float32),
            pltpu.SemaphoreType.DMA((2, tiles)),
            pltpu.SemaphoreType.DMA(()),
        ],
        compiler_params=pltpu.CompilerParams(vmem_limit_bytes=16 * 2**20),
        cost_estimate=pl.CostEstimate(
            flops=6 * rows * cols, bytes_accessed=18 * rows * cols, transcendentals=0
        ),
    )(factor, outer_params, gradient, momentum, absmax)


def per_device(outer_params, local_params, momentum):
    gradient, momentum, absmax, factor = exchange(outer_params, local_params, momentum)
    return finish(factor, outer_params, gradient, momentum, absmax)


def solution(mesh):
    return jax.shard_map(
        per_device,
        mesh=mesh,
        in_specs=(P("shard", None), P("replica", "shard", None), P("shard", None)),
        out_specs=(P("shard", None), P("shard", None), P(None, "shard")),
        check_vma=False,
    )
```
